32 devices in a mesh: dp: 8 (over z, y), expert: 4 (over x, core).
Axes of the slice: x: 2, y: 2, z: 4, core: 2. Of those that a mesh axis runs over, the one named last changes fastest.
Arguments:
- expert_grads: bfloat16 [8, 4, 1024, 896], P('dp', 'expert'), may hold values from -768 to 768
- round_offsets: int32 [8, 4, 1024], P('dp', 'expert'), may hold values from 0 to 1073741823
- slot_expert: int32 [4], replicated, may hold values from 0 to 3, each once
- master_weight: float32 [4, 1024, 896], P('expert', 'dp'), may hold values from -0.1875 to 0.1875
Outputs:
- mean_grad: float32 [4, 1024, 896], P('expert', 'dp')
- new_weight: float32 [4, 1024, 896], P('expert', 'dp')
- block_step: float32 [4, 8], P('expert', 'dp')
The draws below stay inside these ranges and needn't reach their ends.
Inputs may be any that keep to these rules, and one draw needn't show every extreme that they name: `slot_expert`: each of 0 to 3 appears once.
All inputs are finite; a program needn't handle non-finite values.
Results may differ from the reference program's by a relative error of at most 0.0003.
Values may be sent and summed in bfloat16 or wider, within the bound.
A program may use at most 64 MiB of HBM per device.

```python
import jax
import jax.numpy as jnp
from jax import lax

D = 1024
FF = 896
EXPERTS = 4
REPLICAS = 8
N_DP = 8


def draw_expert_grads(key, part):
    base_key = jax.random.fold_in(key, 11)
    scale_key = jax.random.fold_in(key, 12)
    pair_key = jax.random.fold_in(key, 13)
    block_count = REPLICAS
    block_rows = D // REPLICAS
    base = jnp.clip(jax.random.normal(base_key, (REPLICAS, EXPERTS, D, FF), jnp.float32), -4.0, 4.0)
    block_scale = jnp.exp(jax.random.uniform(scale_key, (EXPERTS, block_count), jnp.float32, jnp.log(0.5), jnp.log(32.0)))
    row_scale = jnp.repeat(block_scale, block_rows, axis=1)
    paired = jax.random.permutation(pair_key, block_count)
    blocks_iota = jnp.arange(block_count)
    spike = jnp.where(blocks_iota[None, :] == paired[:, None], jnp.float32(6.0), jnp.float32(1.0))
    row_spike = jnp.repeat(spike, block_rows, axis=1)
    values = base * row_scale[None, :, :, None] * row_spike[:, None, :, None]
    return values.astype(jnp.bfloat16)


def with_ends(drawn, own_key, smallest, high):
    longest = drawn.shape.index(max(drawn.shape))
    spots = []
    for shift in (0, 1):
        where = [jax.random.randint(jax.random.fold_in(own_key, axis), (), 0, length) for axis, length in enumerate(drawn.shape)]
        where[longest] = (where[longest] + shift) % drawn.shape[longest]
        spots.append(tuple(where))
    return drawn.at[spots[0]].set(smallest).at[spots[1]].set(high)


def steps_of(own_key, extent, pieces, smallest, top_value):
    gain = 1.0
    for dim, blocks in pieces:
        draws = jax.random.uniform(jax.random.fold_in(jax.random.fold_in(own_key, 6), dim), (blocks,), jnp.float32, smallest / len(pieces), top_value / len(pieces))
        gain = gain * jnp.repeat(jnp.exp(draws), extent[dim] // blocks).reshape((-1,) + (1,) * (len(extent) - 1 - dim))
    return gain


def gaussian(key, shape, deviation, limit, pieces=(), held_as=jnp.bfloat16):
    level = steps_of(key, shape, pieces, -0.22, 0.18) if pieces else 1.0
    values = jax.random.normal(key, shape, jnp.float32) * deviation * level
    return jnp.minimum(jnp.maximum(values, -limit), limit).astype(held_as)


def setup_inputs(seed: int = 0) -> dict:
    key_of = jax.random.split(jax.random.key(seed), 5)
    return {
        "expert_grads": draw_expert_grads(jax.random.fold_in(key_of[4], 71), 0),
        "round_offsets": with_ends(jax.random.randint(key_of[1], (REPLICAS, EXPERTS, D), 0, 2 ** 30), jax.random.fold_in(key_of[1], 1), 0, (2 ** 30) - 1).astype(jnp.int32),
        "slot_expert": jax.random.permutation(key_of[2], EXPERTS).astype(jnp.int32),
        "master_weight": gaussian(key_of[3], (EXPERTS, D, FF), D ** -0.5, 0.1875, ((0, 4), (1, 8)), jnp.float32),
    }


level_bits = 6
low_power = -30
high_power = 30
learn_rate = 0.05


def power_steps(maxima):
    powers = jnp.array([2.0 ** exponent for exponent in range(low_power, high_power)], jnp.float32)
    reached = maxima[..., None] >= powers
    doubled = jnp.prod(jnp.where(reached, jnp.float32(2.0), jnp.float32(1.0)), axis=-1)
    return (2.0 ** (low_power - level_bits)) * doubled


def dither(element_code):
    mixed = element_code * 747796405 + 1013904223
    mixed = jnp.bitwise_xor(mixed, jnp.right_shift(mixed, 13))
    mixed = mixed * 1103515245
    mixed = jnp.bitwise_xor(mixed, jnp.right_shift(mixed, 16))
    return jnp.bitwise_and(jnp.right_shift(mixed, 12), 255).astype(jnp.float32) / 256.0


def quantize(values, inverse_step, offsets):
    columns = lax.broadcasted_iota(jnp.int32, (1, values.shape[-1]), 1)
    element_code = offsets.astype(jnp.int32)[..., None] + columns
    scaled = values * inverse_step
    floor_part = jnp.floor(scaled)
    return (floor_part + jnp.floor((scaled - floor_part) + dither(element_code))).astype(jnp.int32)


def reference(expert_grads, round_offsets, slot_expert, master_weight):
    slot_count = expert_grads.shape[1]
    row_count = expert_grads.shape[2]
    hidden = expert_grads.shape[3]
    blocks = N_DP
    block_rows = row_count // blocks

    def max_step(running, grads_one):
        shaped = jnp.abs(grads_one).reshape(slot_count, blocks, block_rows, hidden)
        return jnp.maximum(running, jnp.max(shaped, axis=(2, 3)).astype(jnp.float32)), None

    maxima, ignored = lax.scan(max_step, jnp.zeros((slot_count, blocks), jnp.float32), expert_grads)
    step_sizes = power_steps(maxima)
    inverse_step = (1.0 / step_sizes)[:, :, None, None]

    def sum_step(running, grads_pair):
        grads_one, offsets_one = grads_pair
        shaped = grads_one.astype(jnp.float32).reshape(slot_count, blocks, block_rows, hidden)
        offsets_shaped = offsets_one.reshape(slot_count, blocks, block_rows)
        counts = quantize(shaped, inverse_step, offsets_shaped).reshape(slot_count, row_count, hidden)
        return running + counts, None

    totals, ignored = lax.scan(sum_step, jnp.zeros((slot_count, row_count, hidden), jnp.int32), (expert_grads, round_offsets))
    shaped_totals = totals.astype(jnp.float32).reshape(slot_count, blocks, block_rows, hidden)
    mean_slot = (shaped_totals * (step_sizes / N_DP)[:, :, None, None]).reshape(slot_count, row_count, hidden)
    inverse_order = jnp.argsort(slot_expert).astype(jnp.int32)
    mean_grad = mean_slot[inverse_order]
    block_step = step_sizes[inverse_order]
    new_weight = master_weight - learn_rate * mean_grad
    return mean_grad, new_weight, block_step
```

```python
import functools

import jax
import jax.numpy as jnp
from jax import lax
from jax.experimental import pallas as pl
from jax.experimental.pallas import tpu as pltpu
from jax.sharding import PartitionSpec as P

level_bits = 6
low_power = -30
high_power = 30
learn_rate = 0.05
field_base = 32768
count_shift = 64


def power_steps(maxima):
    powers = jnp.array([2.0**exponent for exponent in range(low_power, high_power)], jnp.float32)
    reached = maxima[..., None] >= powers
    doubled = jnp.prod(jnp.where(reached, jnp.float32(2.0), jnp.float32(1.0)), axis=-1)
    return 2.0 ** (low_power - level_bits) * doubled


def dither(element_code):
    mixed = element_code * 747796405 + 1013904223
    mixed = jnp.bitwise_xor(mixed, jnp.right_shift(mixed, 13))
    mixed = mixed * 1103515245
    mixed = jnp.bitwise_xor(mixed, jnp.right_shift(mixed, 16))
    return jnp.bitwise_and(jnp.right_shift(mixed, 12), 255).astype(jnp.float32) / 256.0


def quantize(values, inverse_step, offsets):
    columns = lax.broadcasted_iota(jnp.int32, (1, values.shape[-1]), 1)
    element_code = offsets[..., None] + columns
    scaled = values * inverse_step
    floor_part = jnp.floor(scaled)
    return (floor_part + jnp.floor(scaled - floor_part + dither(element_code))).astype(jnp.int32)


def local_counts(local_grads, round_offsets, all_steps, dp_count):
    slot_count = local_grads.shape[0]
    row_count = local_grads.shape[1]
    hidden = local_grads.shape[2]
    block_rows = row_count // dp_count
    shaped = local_grads.reshape(slot_count, dp_count, block_rows, hidden)
    offsets_shaped = round_offsets[0].reshape(slot_count, dp_count, block_rows)
    counts = quantize(
        shaped.astype(jnp.float32), (1.0 / all_steps)[:, :, None, None], offsets_shaped
    )
    return counts.reshape(slot_count, row_count, hidden)


def block_peaks(local_grads, dp_count):
    slot_count = local_grads.shape[0]
    row_count = local_grads.shape[1]
    hidden = local_grads.shape[2]
    shaped = local_grads.reshape(slot_count, dp_count, row_count // dp_count, hidden)
    return jnp.max(jnp.abs(shaped), axis=(2, 3)).astype(jnp.float32)


def body(expert_grads, round_offsets, slot_expert, master_weight):
    dp_count = lax.axis_size("dp")
    local_grads = expert_grads[0]
    slot_count = local_grads.shape[0]
    hidden = local_grads.shape[2]
    maxima = lax.pmax(block_peaks(local_grads, dp_count), "dp")
    all_steps = power_steps(maxima)
    counts = local_counts(local_grads, round_offsets, all_steps, dp_count)
    half = hidden // 2
    words = (counts[:, :, :half] + count_shift) * field_base + (counts[:, :, half:] + count_shift)
    summed = lax.psum_scatter(words, "dp", scatter_dimension=1, tiled=True)
    upper = jnp.right_shift(summed, 15) - count_shift * dp_count
    lower = jnp.bitwise_and(summed, field_base - 1) - count_shift * dp_count
    totals = jnp.concatenate([upper, lower], axis=2)
    step_sizes = lax.dynamic_slice_in_dim(all_steps, lax.axis_index("dp"), 1, 1)
    mean_slot = totals.astype(jnp.float32) * (step_sizes / dp_count)[..., None]
    gathered, gathered_steps = (
        lax.all_gather(mean_slot, "expert", axis=0, tiled=True),
        lax.all_gather(step_sizes, "expert", axis=0, tiled=True),
    )
    wanted = lax.axis_index("expert") * slot_count + lax.broadcasted_iota(
        jnp.int32, (slot_count, 1), 0
    )
    positions = lax.broadcasted_iota(jnp.int32, (1, slot_expert.shape[0]), 1)
    holder = jnp.sum(jnp.where(slot_expert[None, :] == wanted, positions, 0), axis=1)
    mean_grad = gathered[holder]
    block_step = gathered_steps[holder]
    new_weight = master_weight - learn_rate * mean_grad
    return (mean_grad, new_weight, block_step)


lanes = 128
chunk_rows = 16
MESH = pl.DeviceIdType.MESH


def mixed_dither(code):
    mixed = jnp.bitwise_xor(code, jnp.right_shift(code, 13))
    mixed = mixed * 1103515245
    mixed = jnp.bitwise_xor(mixed, jnp.right_shift(mixed, 16))
    return jnp.bitwise_and(jnp.right_shift(mixed, 12), 255).astype(jnp.float32) * (1.0 / 256.0)


def exchange_kernel(
    n_dp,
    n_expert,
    slots_ref,
    grads_ref,
    offs_ref,
    total_ref,
    step_ref,
    own,
    peer_raw,
    peer_offs,
    codes,
    my_max,
    max_in,
    inverse,
    my_step,
    step_in,
    stage,
    z_in,
    x_out,
    x_in,
    load_sem,
    y_send,
    y_recv,
    z_send,
    z_recv,
    x_send,
    x_recv,
    m_send,
    m_recv,
    o_send,
    o_recv,
    s_send,
    s_recv,
):
    lead = n_dp // 2
    block_rows = own.shape[1]
    hidden = own.shape[2]
    tiles = hidden // lanes
    chunks = block_rows // chunk_rows
    me = lax.axis_index("dp")
    mine = lax.axis_index("expert")
    row = lax.div(me, 2)
    side = lax.rem(me, 2)
    partner = me + 1 - 2 * side

    def rows_of(c):
        return pl.ds(pl.multiple_of(c * chunk_rows, chunk_rows), chunk_rows)

    def dp_peer(d):
        return lax.rem(me + d, n_dp)

    def row_peer(d):
        return lax.rem(row + d, lead)

    def expert_peer(d):
        return lax.rem(mine + d, n_expert)

    def load_copy(b):
        return pltpu.make_async_copy(
            grads_ref.at[lax.div(b, 2), lax.rem(b, 2)], own.at[b], load_sem.at[b]
        )

    def remote(src, dst, send, recv, dp, expert):
        return pltpu.make_async_remote_copy(
            src_ref=src,
            dst_ref=dst,
            send_sem=send,
            recv_sem=recv,
            device_id=(dp, expert),
            device_id_type=MESH,
        )

    def y_copy(c):
        return remote(
            grads_ref.at[:, 1 - side, rows_of(c), :],
            peer_raw.at[c],
            y_send.at[c],
            y_recv.at[c],
            partner,
            mine,
        )

    def z_copy(d, c):
        return remote(
            stage.at[d, rows_of(c), :],
            z_in.at[d - 1, rows_of(c), :],
            z_send.at[d - 1, c],
            z_recv.at[d - 1, c],
            row_peer(d) * 2 + side,
            mine,
        )

    def x_copy(d, c):
        return remote(
            x_out.at[rows_of(c), :],
            x_in.at[d - 1, rows_of(c), :],
            x_send.at[d - 1, c],
            x_recv.at[d - 1, c],
            me,
            expert_peer(d),
        )

    def m_copy(d):
        return remote(
            my_max, max_in.at[d - 1], m_send.at[d - 1], m_recv.at[d - 1], dp_peer(d), mine
        )

    def s_copy(d):
        return remote(
            my_step, step_in.at[d - 1], s_send.at[d - 1], s_recv.at[d - 1], me, expert_peer(d)
        )

    o_copy = remote(offs_ref, peer_offs, o_send, o_recv, partner, mine)

    for b in range(n_dp):
        load_copy(b).start()
    barrier = pltpu.get_barrier_semaphore()
    for d in range(1, n_dp):
        pl.semaphore_signal(barrier, inc=1, device_id=(dp_peer(d), mine), device_id_type=MESH)
    for d in range(1, n_expert):
        pl.semaphore_signal(barrier, inc=1, device_id=(me, expert_peer(d)), device_id_type=MESH)

    block_of_row = lax.broadcasted_iota(jnp.int32, (n_dp, lanes), 0)
    peaks = jnp.zeros((n_dp, lanes), jnp.float32)
    for b in range(n_dp):
        load_copy(b).wait()

        def peak_rows(i, peak):
            return jnp.maximum(peak, jnp.abs(own[b, rows_of(i), :]))

        peak = lax.fori_loop(
            0, chunks, peak_rows, jnp.zeros((chunk_rows, hidden), own.dtype), unroll=True
        ).astype(jnp.float32)
        peak = jnp.max(jnp.max(peak, axis=0, keepdims=True), axis=1, keepdims=True)
        peaks = jnp.where(block_of_row == b, peak, peaks)
    my_max[...] = peaks

    pl.semaphore_wait(barrier, n_dp + n_expert - 2)
    for d in range(1, n_dp):
        m_copy(d).start()
    o_copy.start()
    for c in range(chunks):
        y_copy(c).start()

    def spread(source, slot):
        lines = source[...]
        for k in range(lead):
            line = jnp.where(side == 0, lines[2 * k : 2 * k + 1], lines[2 * k + 1 : 2 * k + 2])
            column = jnp.transpose(jnp.broadcast_to(line, (lanes, block_rows)))
            codes[slot, k] = column * 747796405 + 1013904223

    spread(offs_ref, 0)
    o_copy.wait_recv()
    spread(peer_offs, 1)

    peak = my_max[...]
    for d in range(1, n_dp):
        m_copy(d).wait_recv()
        peak = jnp.maximum(peak, max_in[d - 1])
    step = jnp.full(peak.shape, 2.0 ** (low_power - level_bits), jnp.float32)
    inv = jnp.full(peak.shape, 2.0 ** (level_bits - low_power), jnp.float32)
    for k in range(low_power, high_power):
        reached = peak >= 2.0**k
        step = jnp.where(reached, 2.0 ** (k + 1 - level_bits), step)
        inv = jnp.where(reached, 2.0 ** (level_bits - k - 1), inv)
    my_step[...] = step
    for b in range(n_dp):
        inverse[b] = jnp.broadcast_to(inv[b : b + 1], (chunk_rows, lanes))

    columns = lax.broadcasted_iota(jnp.int32, (chunk_rows, hidden), 1) * 747796405

    def quantized(values, inv_row, code):
        scaled = values.astype(jnp.float32) * inv_row
        floor_part = jnp.floor(scaled)
        wide = jnp.concatenate([code] * tiles, axis=1)
        return floor_part + jnp.floor((scaled - floor_part) + mixed_dither(wide + columns))

    def round_and_send(c):
        y_copy(c).wait_recv()

        def one(i, carry):
            d = lax.rem(i + 1, lead)
            k = row_peer(d)
            b = 2 * k + side
            inv_row = jnp.concatenate([inverse[b]] * tiles, axis=1)
            here = quantized(own[b, rows_of(c), :], inv_row, codes[0, k, rows_of(c), :])
            there = quantized(peer_raw[c, k], inv_row, codes[1, k, rows_of(c), :])
            stage[d, rows_of(c), :] = (here + there).astype(stage.dtype)
            return carry

        lax.fori_loop(0, lead, one, 0)
        for d in range(1, lead):
            z_copy(d, c).start()

    def add_and_send(c):
        total = stage[0, rows_of(c), :].astype(jnp.float32)
        for d in range(1, lead):
            z_copy(d, c).wait_recv()
            total = total + z_in[d - 1, rows_of(c), :].astype(jnp.float32)
        x_out[rows_of(c), :] = total.astype(jnp.int32).astype(x_out.dtype)
        for d in range(1, n_expert):
            x_copy(d, c).start()

    def weight_of(slot):
        return jnp.where(slots_ref[slot] == mine, jnp.float32(1.0), jnp.float32(0.0))

    weights = [weight_of(lax.rem(mine + n_expert - d, n_expert)) for d in range(n_expert)]

    def select(c):
        chosen = x_out[rows_of(c), :].astype(jnp.int32).astype(jnp.float32) * weights[0]
        for d in range(1, n_expert):
            x_copy(d, c).wait_recv()
            part = x_in[d - 1, rows_of(c), :].astype(jnp.int32).astype(jnp.float32)
            chosen = chosen + part * weights[d]
        total_ref[rows_of(c), :] = chosen

    lag_add = min(2, chunks)
    lag_select = min(3, chunks)
    for t in range(chunks + lag_select):
        if t < chunks:
            round_and_send(t)
        if t == 0:
            for d in range(1, n_expert):
                s_copy(d).start()
        if 0 <= t - lag_add < chunks:
            add_and_send(t - lag_add)
        if 0 <= t - lag_select < chunks:
            select(t - lag_select)

    chosen_step = my_step[...] * weights[0]
    for d in range(1, n_expert):
        s_copy(d).wait_recv()
        chosen_step = chosen_step + step_in[d - 1] * weights[d]
    held = jnp.where(block_of_row == me, chosen_step, 0.0)
    step_ref[...] = jnp.broadcast_to(jnp.max(held, axis=0, keepdims=True), held.shape)

    for d in range(1, n_dp):
        m_copy(d).wait_send()
    o_copy.wait_send()
    for d in range(1, n_expert):
        s_copy(d).wait_send()
    for c in range(chunks):
        y_copy(c).wait_send()
        for d in range(1, lead):
            z_copy(d, c).wait_send()
        for d in range(1, n_expert):
            x_copy(d, c).wait_send()


def apply_kernel(n_dp, total_ref, step_ref, master_ref, mean_ref, weight_ref, block_step_ref):
    step = step_ref[0:1, 0:1]
    mean = total_ref[...] * (step / n_dp)
    mean_ref[0] = mean
    weight_ref[0] = master_ref[0] - learn_rate * mean
    block_step_ref[...] = step


def exchange_body(n_dp, n_expert, expert_grads, round_offsets, slot_expert, master_weight):
    row_count, hidden = expert_grads.shape[2:]
    lead = n_dp // 2
    block_rows = row_count // n_dp
    chunks = block_rows // chunk_rows
    grads = expert_grads.reshape(lead, 2, block_rows, hidden)
    offs = round_offsets.reshape(n_dp, block_rows)
    dma = pltpu.SemaphoreType.DMA
    bf16 = jnp.bfloat16
    vmem = pl.BlockSpec(memory_space=pltpu.VMEM)
    totals, steps = pl.pallas_call(
        functools.partial(exchange_kernel, n_dp, n_expert),
        out_shape=(
            jax.ShapeDtypeStruct((block_rows, hidden), jnp.float32),
            jax.ShapeDtypeStruct((n_dp, lanes), jnp.float32),
        ),
        in_specs=[
            pl.BlockSpec(memory_space=pltpu.SMEM),
            pl.BlockSpec(memory_space=pl.ANY),
            vmem,
        ],
        out_specs=(vmem, vmem),
        scratch_shapes=[
            pltpu.VMEM((n_dp, block_rows, hidden), bf16),
            pltpu.VMEM((chunks, lead, chunk_rows, hidden), bf16),
            pltpu.VMEM((n_dp, block_rows), jnp.int32),
            pltpu.VMEM((2, lead, block_rows, lanes), jnp.int32),
            pltpu.VMEM((n_dp, lanes), jnp.float32),
            pltpu.VMEM((n_dp - 1, n_dp, lanes), jnp.float32),
            pltpu.VMEM((n_dp, chunk_rows, lanes), jnp.float32),
            pltpu.VMEM((n_dp, lanes), jnp.float32),
            pltpu.VMEM((n_expert - 1, n_dp, lanes), jnp.float32),
            pltpu.VMEM((lead, block_rows, hidden), bf16),
            pltpu.VMEM((lead - 1, block_rows, hidden), bf16),
            pltpu.VMEM((block_rows, hidden), jnp.int16),
            pltpu.VMEM((n_expert - 1, block_rows, hidden), jnp.int16),
            dma((n_dp,)),
            dma((chunks,)),
            dma((chunks,)),
            dma((lead - 1, chunks)),
            dma((lead - 1, chunks)),
            dma((n_expert - 1, chunks)),
            dma((n_expert - 1, chunks)),
            dma((n_dp - 1,)),
            dma((n_dp - 1,)),
            dma,
            dma,
            dma((n_expert - 1,)),
            dma((n_expert - 1,)),
        ],
        compiler_params=pltpu.CompilerParams(collective_id=0, has_side_effects=True),
    )(slot_expert, grads, offs)
    return pl.pallas_call(
        functools.partial(apply_kernel, n_dp),
        out_shape=(
            jax.ShapeDtypeStruct(master_weight.shape, jnp.float32),
            jax.ShapeDtypeStruct(master_weight.shape, jnp.float32),
            jax.ShapeDtypeStruct((1, 1), jnp.float32),
        ),
        in_specs=[vmem, vmem, vmem],
        out_specs=(vmem, vmem, vmem),
    )(totals, steps, master_weight)


def solution(mesh):
    n_dp = mesh.shape["dp"]
    n_expert = mesh.shape["expert"]

    def routed(expert_grads, round_offsets, slot_expert, master_weight):
        slot_count, row_count, hidden = expert_grads.shape[1:]
        block_rows = row_count // n_dp
        fits = (
            slot_count == 1
            and n_expert > 1
            and n_dp >= 4
            and n_dp % 2 == 0
            and block_rows == lanes
            and hidden % lanes == 0
        )
        if fits:
            return exchange_body(
                n_dp, n_expert, expert_grads, round_offsets, slot_expert, master_weight
            )
        return body(expert_grads, round_offsets, slot_expert, master_weight)

    return jax.shard_map(
        routed,
        mesh=mesh,
        in_specs=(
            P("dp", "expert", None, None),
            P("dp", "expert", None),
            P(),
            P("expert", "dp", None),
        ),
        out_specs=(P("expert", "dp", None), P("expert", "dp", None), P("expert", "dp")),
        check_vma=False,
    )
```

```python
import functools

import jax
import jax.numpy as jnp
from jax import lax
from jax.experimental import pallas as pl
from jax.experimental.pallas import tpu as pltpu
from jax.sharding import PartitionSpec as P

level_bits = 6
low_power = -30
high_power = 30
learn_rate = 0.05
field_base = 32768
count_shift = 64


def power_steps(maxima):
    powers = jnp.array([2.0**exponent for exponent in range(low_power, high_power)], jnp.float32)
    reached = maxima[..., None] >= powers
    doubled = jnp.prod(jnp.where(reached, jnp.float32(2.0), jnp.float32(1.0)), axis=-1)
    return 2.0 ** (low_power - level_bits) * doubled


def dither(element_code):
    mixed = element_code * 747796405 + 1013904223
    mixed = jnp.bitwise_xor(mixed, jnp.right_shift(mixed, 13))
    mixed = mixed * 1103515245
    mixed = jnp.bitwise_xor(mixed, jnp.right_shift(mixed, 16))
    return jnp.bitwise_and(jnp.right_shift(mixed, 12), 255).astype(jnp.float32) / 256.0


def quantize(values, inverse_step, offsets):
    columns = lax.broadcasted_iota(jnp.int32, (1, values.shape[-1]), 1)
    element_code = offsets[..., None] + columns
    scaled = values * inverse_step
    floor_part = jnp.floor(scaled)
    return (floor_part + jnp.floor(scaled - floor_part + dither(element_code))).astype(jnp.int32)


def local_counts(local_grads, round_offsets, all_steps, dp_count):
    slot_count = local_grads.shape[0]
    row_count = local_grads.shape[1]
    hidden = local_grads.shape[2]
    block_rows = row_count // dp_count
    shaped = local_grads.reshape(slot_count, dp_count, block_rows, hidden)
    offsets_shaped = round_offsets[0].reshape(slot_count, dp_count, block_rows)
    counts = quantize(
        shaped.astype(jnp.float32), (1.0 / all_steps)[:, :, None, None], offsets_shaped
    )
    return counts.reshape(slot_count, row_count, hidden)


def block_peaks(local_grads, dp_count):
    slot_count = local_grads.shape[0]
    row_count = local_grads.shape[1]
    hidden = local_grads.shape[2]
    shaped = local_grads.reshape(slot_count, dp_count, row_count // dp_count, hidden)
    return jnp.max(jnp.abs(shaped), axis=(2, 3)).astype(jnp.float32)


def body(expert_grads, round_offsets, slot_expert, master_weight):
    dp_count = lax.axis_size("dp")
    local_grads = expert_grads[0]
    slot_count = local_grads.shape[0]
    hidden = local_grads.shape[2]
    maxima = lax.pmax(block_peaks(local_grads, dp_count), "dp")
    all_steps = power_steps(maxima)
    counts = local_counts(local_grads, round_offsets, all_steps, dp_count)
    half = hidden // 2
    words = (counts[:, :, :half] + count_shift) * field_base + (counts[:, :, half:] + count_shift)
    summed = lax.psum_scatter(words, "dp", scatter_dimension=1, tiled=True)
    upper = jnp.right_shift(summed, 15) - count_shift * dp_count
    lower = jnp.bitwise_and(summed, field_base - 1) - count_shift * dp_count
    totals = jnp.concatenate([upper, lower], axis=2)
    step_sizes = lax.dynamic_slice_in_dim(all_steps, lax.axis_index("dp"), 1, 1)
    mean_slot = totals.astype(jnp.float32) * (step_sizes / dp_count)[..., None]
    gathered, gathered_steps = (
        lax.all_gather(mean_slot, "expert", axis=0, tiled=True),
        lax.all_gather(step_sizes, "expert", axis=0, tiled=True),
    )
    wanted = lax.axis_index("expert") * slot_count + lax.broadcasted_iota(
        jnp.int32, (slot_count, 1), 0
    )
    positions = lax.broadcasted_iota(jnp.int32, (1, slot_expert.shape[0]), 1)
    holder = jnp.sum(jnp.where(slot_expert[None, :] == wanted, positions, 0), axis=1)
    mean_grad = gathered[holder]
    block_step = gathered_steps[holder]
    new_weight = master_weight - learn_rate * mean_grad
    return (mean_grad, new_weight, block_step)


lanes = 128
chunk_rows = 16
MESH = pl.DeviceIdType.MESH


def mixed_dither(code):
    mixed = jnp.bitwise_xor(code, jnp.right_shift(code, 13))
    mixed = mixed * 1103515245
    mixed = jnp.bitwise_xor(mixed, jnp.right_shift(mixed, 16))
    return jnp.bitwise_and(jnp.right_shift(mixed, 12), 255).astype(jnp.float32) * (1.0 / 256.0)


def exchange_kernel(
    n_dp,
    n_expert,
    slots_ref,
    grads_ref,
    offs_ref,
    total_ref,
    step_ref,
    own,
    peer_raw,
    peer_offs,
    codes,
    my_max,
    max_in,
    inverse,
    my_step,
    step_in,
    stage,
    z_in,
    x_out,
    x_in,
    first_raw,
    first_offs,
    first_codes,
    first_here,
    first_out,
    first_in,
    load_sem,
    y_send,
    y_recv,
    z_send,
    z_recv,
    x_send,
    x_recv,
    m_send,
    m_recv,
    o_send,
    o_recv,
    s_send,
    s_recv,
    f_send,
    f_recv,
    g_send,
    g_recv,
    p_send,
    p_recv,
):
    lead = n_dp // 2
    block_rows = own.shape[2]
    hidden = own.shape[3]
    tiles = hidden // lanes
    chunks = block_rows // chunk_rows
    me = lax.axis_index("dp")
    mine = lax.axis_index("expert")
    row = lax.div(me, 2)
    side = lax.rem(me, 2)
    partner = me + 1 - 2 * side

    def rows_of(c):
        return pl.ds(pl.multiple_of(c * chunk_rows, chunk_rows), chunk_rows)

    def dp_peer(d):
        return lax.rem(me + d, n_dp)

    def row_peer(d):
        return lax.rem(row + d, lead)

    def expert_peer(d):
        return lax.rem(mine + d, n_expert)

    def load_copy(b):
        return pltpu.make_async_copy(
            grads_ref.at[b // 2, b % 2], own.at[b // 2, b % 2], load_sem.at[b]
        )

    def remote(src, dst, send, recv, dp, expert):
        return pltpu.make_async_remote_copy(
            src_ref=src,
            dst_ref=dst,
            send_sem=send,
            recv_sem=recv,
            device_id=(dp, expert),
            device_id_type=MESH,
        )

    def y_copy(d, c):
        return remote(
            own.at[row_peer(d), 1 - side, rows_of(c), :],
            peer_raw.at[c, d],
            y_send.at[d, c],
            y_recv.at[d, c],
            partner,
            mine,
        )

    def first_copy(d):
        return remote(
            own.at[row_peer(d), :, rows_of(0), :],
            first_raw.at[d - 1],
            f_send.at[d - 1],
            f_recv.at[d - 1],
            row_peer(d) * 2 + side,
            mine,
        )

    def first_offs_copy(d):
        return remote(
            offs_ref,
            first_offs.at[d - 1],
            g_send.at[d - 1],
            g_recv.at[d - 1],
            row_peer(d) * 2 + side,
            mine,
        )

    p_copy = remote(first_out, first_in, p_send, p_recv, partner, mine)

    remote_order = [lead // 2] + [d for d in range(1, lead) if d != lead // 2]

    def y_issue(c):
        for d in remote_order:
            y_copy(d, c).start()
        if c >= 3:
            y_copy(0, c - 2).start()
        if c == chunks - 1:
            y_copy(0, c - 1).start()
            y_copy(0, c).start()

    def z_copy(d, c):
        return remote(
            stage.at[d, rows_of(c), :],
            z_in.at[d - 1, rows_of(c), :],
            z_send.at[d - 1, c],
            z_recv.at[d - 1, c],
            row_peer(d) * 2 + side,
            mine,
        )

    def x_copy(d, c):
        return remote(
            x_out.at[rows_of(c), :],
            x_in.at[d - 1, rows_of(c), :],
            x_send.at[d - 1, c],
            x_recv.at[d - 1, c],
            me,
            expert_peer(d),
        )

    def m_copy(d):
        return remote(
            my_max, max_in.at[d - 1], m_send.at[d - 1], m_recv.at[d - 1], dp_peer(d), mine
        )

    def s_copy(d):
        return remote(
            my_step, step_in.at[d - 1], s_send.at[d - 1], s_recv.at[d - 1], me, expert_peer(d)
        )

    o_copy = remote(offs_ref, peer_offs, o_send, o_recv, partner, mine)

    for b in range(n_dp):
        load_copy(b).start()
    barrier = pltpu.get_barrier_semaphore()
    for d in range(1, n_dp):
        pl.semaphore_signal(barrier, inc=1, device_id=(dp_peer(d), mine), device_id_type=MESH)
    for d in range(1, n_expert):
        pl.semaphore_signal(barrier, inc=1, device_id=(me, expert_peer(d)), device_id_type=MESH)

    block_of_row = lax.broadcasted_iota(jnp.int32, (n_dp, lanes), 0)
    peaks = jnp.zeros((n_dp, lanes), jnp.float32)
    for b in range(n_dp):
        load_copy(b).wait()

        def peak_rows(i, peak):
            return jnp.maximum(peak, jnp.abs(own[b // 2, b % 2, rows_of(i), :]))

        peak = lax.fori_loop(
            0, chunks, peak_rows, jnp.zeros((chunk_rows, hidden), own.dtype), unroll=True
        ).astype(jnp.float32)
        peak = jnp.max(jnp.max(peak, axis=0, keepdims=True), axis=1, keepdims=True)
        peaks = jnp.where(block_of_row == b, peak, peaks)
    my_max[...] = peaks

    pl.semaphore_wait(barrier, n_dp + n_expert - 2)
    for d in range(1, n_dp):
        m_copy(d).start()
    o_copy.start()
    for d in range(1, lead):
        first_offs_copy(d).start()
    for d in remote_order:
        first_copy(d).start()
    ahead = 4
    for c in range(1, 1 + ahead):
        y_issue(c)

    def spread(source, slot):
        lines = source[...]
        for k in range(lead):
            line = jnp.where(side == 0, lines[2 * k : 2 * k + 1], lines[2 * k + 1 : 2 * k + 2])
            column = jnp.transpose(jnp.broadcast_to(line, (lanes, block_rows)))
            codes[slot, k] = column * 747796405 + 1013904223

    spread(offs_ref, 0)
    o_copy.wait_recv()
    spread(peer_offs, 1)

    def first_spread(source, slot):
        for at in range(2):
            line = jnp.sum(
                jnp.where(block_of_row == 2 * row + at, source, 0), axis=0, keepdims=True
            )
            column = jnp.transpose(jnp.broadcast_to(line, (lanes, block_rows)))[:chunk_rows]
            first_codes[slot, at] = column * 747796405 + 1013904223

    first_spread(offs_ref[...], 0)

    peak = my_max[...]
    for d in range(1, n_dp):
        m_copy(d).wait_recv()
        peak = jnp.maximum(peak, max_in[d - 1])
    step = jnp.full(peak.shape, 2.0 ** (low_power - level_bits), jnp.float32)
    inv = jnp.full(peak.shape, 2.0 ** (level_bits - low_power), jnp.float32)
    for k in range(low_power, high_power):
        reached = peak >= 2.0**k
        step = jnp.where(reached, 2.0 ** (k + 1 - level_bits), step)
        inv = jnp.where(reached, 2.0 ** (level_bits - k - 1), inv)
    my_step[...] = step
    for b in range(n_dp):
        inverse[b] = jnp.broadcast_to(inv[b : b + 1], (chunk_rows, lanes))

    columns = lax.broadcasted_iota(jnp.int32, (chunk_rows, hidden), 1) * 747796405

    def quantized(values, inv_row, code):
        scaled = values.astype(jnp.float32) * inv_row
        floor_part = jnp.floor(scaled)
        wide = jnp.concatenate([code] * tiles, axis=1)
        return floor_part + jnp.floor((scaled - floor_part) + mixed_dither(wide + columns))

    def round_piece(d, c):
        y_copy(d, c).wait_recv()
        k = row_peer(d)
        inv_row = jnp.concatenate([inverse[2 * k + side]] * tiles, axis=1)
        here = quantized(own[k, side, rows_of(c), :], inv_row, codes[0, k, rows_of(c), :])
        there = quantized(peer_raw[c, d], inv_row, codes[1, k, rows_of(c), :])
        stage[d, rows_of(c), :] = (here + there).astype(stage.dtype)

    def round_and_send(c):
        last = None
        for d in remote_order:
            round_piece(d, c)
            if last is not None:
                z_copy(last, c).start()
            last = d
        if c >= 4:
            round_piece(0, c - 3)
        z_copy(last, c).start()

    def first_round():
        for d in range(1, lead):
            first_offs_copy(d).wait_recv()
            first_spread(first_offs[d - 1], d)
            first_copy(d).wait_recv()

        def summed(at):
            inv_row = jnp.concatenate([inverse[2 * row + at]] * tiles, axis=1)
            total = quantized(own[row, at, rows_of(0), :], inv_row, first_codes[0, at])

            def one(d, total):
                return total + quantized(first_raw[d - 1, at], inv_row, first_codes[d, at])

            return lax.fori_loop(1, lead, one, total)

        first_out[...] = summed(1 - side).astype(first_out.dtype)
        first_here[...] = summed(side)
        p_copy.start()

    def first_add():
        p_copy.wait_recv()
        total = first_here[...] + first_in[...].astype(jnp.float32)
        x_out[rows_of(0), :] = total.astype(jnp.int32).astype(x_out.dtype)
        for d in range(1, n_expert):
            x_copy(d, 0).start()

    def add_and_send(c):
        total = stage[0, rows_of(c), :].astype(jnp.float32)
        for d in range(1, lead):
            z_copy(d, c).wait_recv()
            total = total + z_in[d - 1, rows_of(c), :].astype(jnp.float32)
        x_out[rows_of(c), :] = total.astype(jnp.int32).astype(x_out.dtype)
        for d in range(1, n_expert):
            x_copy(d, c).start()

    def weight_of(slot):
        return jnp.where(slots_ref[slot] == mine, jnp.float32(1.0), jnp.float32(0.0))

    weights = [weight_of(lax.rem(mine + n_expert - d, n_expert)) for d in range(n_expert)]

    def select(c):
        chosen = x_out[rows_of(c), :].astype(jnp.int32).astype(jnp.float32) * weights[0]
        for d in range(1, n_expert):
            x_copy(d, c).wait_recv()
            part = x_in[d - 1, rows_of(c), :].astype(jnp.int32).astype(jnp.float32)
            chosen = chosen + part * weights[d]
        total_ref[rows_of(c), :] = chosen

    for t in range(1, chunks + 5):
        if t < chunks:
            round_and_send(t)
            if t + ahead < chunks:
                y_issue(t + ahead)
        elif t - 3 < chunks:
            round_piece(0, t - 3)
        if t == 1:
            for d in range(1, n_expert):
                s_copy(d).start()
        if t == 3:
            first_round()
        if 1 <= t - 3 < chunks:
            add_and_send(t - 3)
        if t == 6:
            first_add()
        if 1 <= t - 5 < chunks:
            select(t - 5)
        if t == 8:
            select(0)

    chosen_step = my_step[...] * weights[0]
    for d in range(1, n_expert):
        s_copy(d).wait_recv()
        chosen_step = chosen_step + step_in[d - 1] * weights[d]
    held = jnp.where(block_of_row == me, chosen_step, 0.0)
    step_ref[...] = jnp.broadcast_to(jnp.max(held, axis=0, keepdims=True), held.shape)

    for d in range(1, n_dp):
        m_copy(d).wait_send()
    o_copy.wait_send()
    for d in range(1, n_expert):
        s_copy(d).wait_send()
    p_copy.wait_send()
    for d in range(1, lead):
        first_copy(d).wait_send()
        first_offs_copy(d).wait_send()
    for c in range(chunks):
        for d in range(lead):
            if c > 0:
                y_copy(d, c).wait_send()
            if c > 0 and d > 0:
                z_copy(d, c).wait_send()
        for d in range(1, n_expert):
            x_copy(d, c).wait_send()


def apply_kernel(n_dp, total_ref, step_ref, master_ref, mean_ref, weight_ref, block_step_ref):
    step = step_ref[0:1, 0:1]
    mean = total_ref[...] * (step / n_dp)
    mean_ref[0] = mean
    weight_ref[0] = master_ref[0] - learn_rate * mean
    block_step_ref[...] = step


def exchange_body(n_dp, n_expert, expert_grads, round_offsets, slot_expert, master_weight):
    row_count, hidden = expert_grads.shape[2:]
    lead = n_dp // 2
    block_rows = row_count // n_dp
    chunks = block_rows // chunk_rows
    grads = expert_grads.reshape(lead, 2, block_rows, hidden)
    offs = round_offsets.reshape(n_dp, block_rows)
    dma = pltpu.SemaphoreType.DMA
    bf16 = jnp.bfloat16
    vmem = pl.BlockSpec(memory_space=pltpu.VMEM)
    totals, steps = pl.pallas_call(
        functools.partial(exchange_kernel, n_dp, n_expert),
        out_shape=(
            jax.ShapeDtypeStruct((block_rows, hidden), jnp.float32),
            jax.ShapeDtypeStruct((n_dp, lanes), jnp.float32),
        ),
        in_specs=[
            pl.BlockSpec(memory_space=pltpu.SMEM),
            pl.BlockSpec(memory_space=pltpu.HBM),
            vmem,
        ],
        out_specs=(vmem, vmem),
        scratch_shapes=[
            pltpu.VMEM((lead, 2, block_rows, hidden), bf16),
            pltpu.VMEM((chunks, lead, chunk_rows, hidden), bf16),
            pltpu.VMEM((n_dp, block_rows), jnp.int32),
            pltpu.VMEM((2, lead, block_rows, lanes), jnp.int32),
            pltpu.VMEM((n_dp, lanes), jnp.float32),
            pltpu.VMEM((n_dp - 1, n_dp, lanes), jnp.float32),
            pltpu.VMEM((n_dp, chunk_rows, lanes), jnp.float32),
            pltpu.VMEM((n_dp, lanes), jnp.float32),
            pltpu.VMEM((n_expert - 1, n_dp, lanes), jnp.float32),
            pltpu.VMEM((lead, block_rows, hidden), bf16),
            pltpu.VMEM((lead - 1, block_rows, hidden), bf16),
            pltpu.VMEM((block_rows, hidden), jnp.int16),
            pltpu.VMEM((n_expert - 1, block_rows, hidden), jnp.int16),
            pltpu.VMEM((lead - 1, 2, chunk_rows, hidden), bf16),
            pltpu.VMEM((lead - 1, n_dp, block_rows), jnp.int32),
            pltpu.VMEM((lead, 2, chunk_rows, lanes), jnp.int32),
            pltpu.VMEM((chunk_rows, hidden), jnp.float32),
            pltpu.VMEM((chunk_rows, hidden), bf16),
            pltpu.VMEM((chunk_rows, hidden), bf16),
            dma((n_dp,)),
            dma((lead, chunks)),
            dma((lead, chunks)),
            dma((lead - 1, chunks)),
            dma((lead - 1, chunks)),
            dma((n_expert - 1, chunks)),
            dma((n_expert - 1, chunks)),
            dma((n_dp - 1,)),
            dma((n_dp - 1,)),
            dma,
            dma,
            dma((n_expert - 1,)),
            dma((n_expert - 1,)),
            dma((lead - 1,)),
            dma((lead - 1,)),
            dma((lead - 1,)),
            dma((lead - 1,)),
            dma,
            dma,
        ],
        compiler_params=pltpu.CompilerParams(
            collective_id=0, has_side_effects=True
        ),
    )(slot_expert, grads, offs)
    return pl.pallas_call(
        functools.partial(apply_kernel, n_dp),
        out_shape=(
            jax.ShapeDtypeStruct(master_weight.shape, jnp.float32),
            jax.ShapeDtypeStruct(master_weight.shape, jnp.float32),
            jax.ShapeDtypeStruct((1, 1), jnp.float32),
        ),
        in_specs=[vmem, vmem, vmem],
        out_specs=(vmem, vmem, vmem),
    )(totals, steps, master_weight)


def solution(mesh):
    n_dp = mesh.shape["dp"]
    n_expert = mesh.shape["expert"]

    def routed(expert_grads, round_offsets, slot_expert, master_weight):
        slot_count, row_count, hidden = expert_grads.shape[1:]
        block_rows = row_count // n_dp
        fits = (
            slot_count == 1
            and n_expert > 1
            and n_dp >= 4
            and n_dp % 2 == 0
            and n_dp <= 8
            and block_rows == lanes
            and hidden % lanes == 0
        )
        if fits:
            return exchange_body(
                n_dp, n_expert, expert_grads, round_offsets, slot_expert, master_weight
            )
        return body(expert_grads, round_offsets, slot_expert, master_weight)

    return jax.shard_map(
        routed,
        mesh=mesh,
        in_specs=(
            P("dp", "expert", None, None),
            P("dp", "expert", None),
            P(),
            P("expert", "dp", None),
        ),
        out_specs=(P("expert", "dp", None), P("expert", "dp", None), P("expert", "dp")),
        check_vma=False,
    )
```
